128 devices in a mesh: fsdp: 8 (over x, y_lo), tensor: 16 (over z, y_hi, core).
Axes of the slice: x: 4, y: 4 (y_hi: 2, y_lo: 2; y = y_hi * 2 + y_lo), z: 4, core: 2. Of those that a mesh axis runs over, the one named last changes fastest.
Arguments:
- modality: int32 [8192], P('fsdp'), may hold values from 0 to 2, as said below
- out_grad: bfloat16 [8192, 4096], P('fsdp', 'tensor'), may hold values from -6 to 6
- gate_pre: bfloat16 [8192, 11008], P('fsdp', 'tensor'), may hold values from -6 to 6
- up_pre: bfloat16 [8192, 11008], P('fsdp', 'tensor'), may hold values from -6 to 6
- down_weight: bfloat16 [3, 11008, 4096], P(None, 'tensor', 'fsdp'), may hold values from -0.0546875 to 0.0546875
Outputs:
- down_grad: float32 [3, 11008, 4096], P(None, 'tensor', 'fsdp')
- gate_grad: bfloat16 [8192, 11008], P('fsdp', 'tensor')
- up_grad: bfloat16 [8192, 11008], P('fsdp', 'tensor')
The draws below stay inside these ranges and needn't reach their ends.
Inputs may be any that keep to these rules, and one draw needn't show every extreme that they name: `modality`: the 1024 tokens of every index of fsdp hold each of the three modalities at least once.
All inputs are finite; a program needn't handle non-finite values.
Results may differ from the reference program's by a relative error of at most 0.012.
Values may be sent and summed in bfloat16 or wider, within the bound.
A program may use at most 256 MiB of HBM per device.

```python
import jax
import jax.numpy as jnp
from jax import lax

D = 4096
FF = 11008
TOK_DEV = 1024
TOKENS = 8192
N_FSDP = 8


def draw_modality(key, part):
    subkeys = jax.random.split(jax.random.fold_in(key, 11), 4)
    groups = TOKENS // TOK_DEV
    position = jnp.arange(TOKENS, dtype=jnp.int32)
    group_id = position // TOK_DEV
    local_pos = position % TOK_DEV
    rotation = jax.random.randint(subkeys[0], (), 0, 3)
    leader = (jnp.arange(groups, dtype=jnp.int32) + rotation) % 3
    shares = jax.random.randint(subkeys[1], (groups,), 3, 9)
    offsets = jax.random.randint(subkeys[2], (groups,), 0, TOK_DEV)
    rolls = jax.random.randint(subkeys[3], (TOKENS,), 0, 20)
    lead_kind = leader[group_id]
    base_kind = jnp.where(rolls < 2 * shares[group_id], lead_kind, (lead_kind + 1 + rolls % 2) % 3)
    distance = (local_pos - offsets[group_id]) % TOK_DEV
    return jnp.where(distance < 3, distance, base_kind).astype(jnp.int32)


def spiked(entries, stream_key, source, target, shards_of, factor):
    owner, partner = [(jnp.arange(entries.shape[axis_at]) // (entries.shape[axis_at] // shards_of)).reshape([-1 if axis == axis_at else 1 for axis in range(entries.ndim)]) for axis_at in (source, target)]
    chosen = jax.random.permutation(stream_key, shards_of)[partner]
    strong = (owner == chosen) | (owner == (partner + shards_of // 2) % shards_of)
    return jnp.where(strong, factor * entries, entries)


def block_scale(rng, shape, pieces, smallest, high):
    def one(dim, shards_of):
        heights = jax.random.uniform(jax.random.fold_in(jax.random.fold_in(rng, 6), dim), (shards_of,), jnp.float32, smallest / len(pieces), high / len(pieces))
        return jnp.repeat(jnp.exp(heights), shape[dim] // shards_of).reshape((-1,) + (1,) * (len(shape) - dim - 1))

    factor_of = one(*pieces[0])
    for cut in pieces[1:]:
        factor_of = factor_of * one(*cut)
    return factor_of


def gaussian(stream_key, shape, deviation, bound, cuts=(), kind=jnp.bfloat16):
    loudness = block_scale(stream_key, shape, cuts, -0.22, 0.18) if cuts else 1.0
    drawn = jax.random.normal(stream_key, shape, jnp.float32) * deviation * loudness
    return jnp.minimum(jnp.maximum(drawn, -bound), bound).astype(kind)


def gaussian_with(own_key, dims, width, bound, cuts, heavy, kind=jnp.bfloat16):
    array = width * jax.random.normal(own_key, dims, jnp.float32)
    if cuts:
        array = array * block_scale(own_key, dims, cuts, -0.22, 0.18)
    return jnp.clip(spiked(array, jax.random.fold_in(own_key, 3), *heavy), -bound, bound).astype(kind)


def setup_inputs(seed: int = 0) -> dict:
    keys = jax.random.split(jax.random.key(seed), 6)
    modality = draw_modality(jax.random.fold_in(keys[5], 71), 0)
    out_grad = gaussian_with(keys[1], (TOKENS, D), 1.0, 6.0, ((0, 8), (1, 16)), (0, 1, 16, 2.0))
    gate_pre = gaussian(keys[2], (TOKENS, FF), 1.0, 6.0, ((0, 8), (1, 16)))
    up_pre = gaussian(keys[3], (TOKENS, FF), 1.0, 6.0, ((0, 8), (1, 16)))
    down_weight = gaussian(keys[4], (3, FF, D), FF ** -0.5, 0.0546875, ((1, 16), (2, 8)))
    return dict(modality=modality, out_grad=out_grad, gate_pre=gate_pre, up_pre=up_pre, down_weight=down_weight)


def reference(modality, out_grad, gate_pre, up_pre, down_weight):
    labels = jnp.arange(3, dtype=jnp.int32)
    kind_onehot = (modality[:, None] == labels[None, :]).astype(jnp.float32)
    counts = jnp.sum(kind_onehot, axis=0)
    factor = TOKENS / (3.0 * counts)
    token_scale = jnp.sum(kind_onehot * factor[None, :], axis=1)
    scaled = (out_grad.astype(jnp.float32) * token_scale[:, None]).astype(jnp.bfloat16)
    gate_val = gate_pre.astype(jnp.float32)
    up_val = up_pre.astype(jnp.float32)
    sigmoid_g = jax.nn.sigmoid(gate_val)
    active = gate_val * sigmoid_g
    hidden = (active * up_val).astype(jnp.bfloat16)
    kind_marks = kind_onehot.T.astype(jnp.bfloat16)
    d_hidden = jnp.zeros((TOKENS, FF), jnp.float32)
    for kind_id in range(3):
        masked = scaled * kind_marks[kind_id][:, None]
        d_hidden = d_hidden + lax.dot_general(masked, down_weight[kind_id], (((1,), (1,)), ((), ())), preferred_element_type=jnp.float32)
    up_grad = (d_hidden * active).astype(jnp.bfloat16)
    slope = sigmoid_g * (1.0 + gate_val * (1.0 - sigmoid_g))
    gate_grad = (d_hidden * up_val * slope).astype(jnp.bfloat16)
    group_hidden = hidden.reshape(N_FSDP, TOK_DEV, FF)
    group_scaled = scaled.reshape(N_FSDP, TOK_DEV, D)
    group_marks = jnp.transpose(kind_marks.reshape(3, N_FSDP, TOK_DEV), (1, 0, 2))

    def one_group(running, group_items):
        rows_hidden, rows_scaled, marks_here = group_items
        partials = []
        for kind_id in range(3):
            masked = rows_scaled * marks_here[kind_id][:, None]
            product = lax.dot_general(rows_hidden, masked, (((0,), (0,)), ((), ())), preferred_element_type=jnp.float32)
            partials.append(lax.optimization_barrier(product.astype(jnp.bfloat16)).astype(jnp.float32))
        return running + jnp.stack(partials), None

    down_grad, _ = lax.scan(one_group, jnp.zeros((3, FF, D), jnp.float32), (group_hidden, group_scaled, group_marks))
    return down_grad, gate_grad, up_grad
```

```python
import jax
import jax.numpy as jnp
from jax import lax
from jax.experimental import pallas as pl
from jax.experimental.pallas import tpu as pltpu
from jax.sharding import Mesh
from jax.sharding import PartitionSpec as P

AXES = ("x", "yl", "z", "yh", "c")
MESH = pl.DeviceIdType.MESH
F32, BF16 = jnp.float32, jnp.bfloat16
S1, YH, ZZ, CC, WW, MM, HR, HL, HFR, HFL = 0, 4, 5, 11, 19, 22, 29, 33, 37, 41
TR, TL, DR1, DL1, DR2, DL2, DW, SEMS = 45, 49, 53, 57, 61, 65, 69, 72


def dot_nt(a, b):
    return lax.dot_general(a, b, (((1,), (1,)), ((), ())), preferred_element_type=F32)


def eye(n):
    same = lax.broadcasted_iota(jnp.int32, (n, n), 0) == lax.broadcasted_iota(jnp.int32, (n, n), 1)
    return same.astype(F32).astype(BF16)


def kernel(
    mod_ref, og_ref, gate_ref, up_ref, w_ref, dw_ref, gg_ref, ug_ref,
    s_ref, wv_ref, ht_ref, part_ref, from_left, from_right, hop_left, hop_right,
    acc_ref, out_half, in_half, gate_v, up_v, mod_all, kind_ref, eye_f, eye_q,
    send, recv, local,
):
    x, yl, z, yh, c = (lax.axis_index(a) for a in AXES)
    rows, ff = gate_ref.shape
    quarter, cols = rows // 4, og_ref.shape[1]
    half = 2 * cols
    total = rows * 8
    cut = (ff // 2 + 15) // 16 * 16
    top, low = pl.ds(0, cut), pl.ds(cut, ff - cut)
    right, left, across = (x + 1) % 4, (x + 3) % 4, (x + 2) % 4
    up_z, down_z = (z + 1) % 4, (z + 3) % 4

    def rc(src, dst, si, ri, **where):
        return pltpu.make_async_remote_copy(
            src_ref=src, dst_ref=dst, send_sem=send.at[si], recv_sem=recv.at[ri],
            device_id=where, device_id_type=MESH,
        )

    def order(k):
        return (z + 3 * k + 3 * (k // 2) + 2 * (k // 3)) % 4

    def tile(i, n):
        return pl.ds(pl.multiple_of(i * n, n), n)

    def s_block(q, e, core):
        return s_ref.at[q, :, tile(((yh + e) % 2) * 2 + core, cols)]

    def w_copy(m):
        return rc(w_ref.at[m], wv_ref.at[m, :, tile(yl, half)], WW + m, WW + m, yl=1 - yl)

    def w_local(m):
        return pltpu.make_async_copy(w_ref.at[m], wv_ref.at[m, :, tile(yl, half)], local.at[2 + m])

    def first_dst(q, source):
        return s_ref.at[q, tile(source, quarter), tile(yh * 2 + c, cols)]

    def first_remote(q):
        return rc(og_ref.at[tile(q, quarter), :], first_dst(q, x), S1 + q, S1 + x, x=z, z=q)

    def is_self(q):
        return jnp.logical_and(x == z, q == z)

    for q in range(4):
        @pl.when(jnp.logical_not(is_self(q)))
        def _():
            first_remote(q).start()

        @pl.when(is_self(q))
        def _():
            pltpu.make_async_copy(
                og_ref.at[tile(q, quarter), :], first_dst(q, x), recv.at[S1 + x]
            ).start()

    w_copy(0).start()
    loads = [
        pltpu.make_async_copy(gate_ref, gate_v, local.at[0]),
        pltpu.make_async_copy(up_ref, up_v, local.at[1]),
    ]
    for copy in loads:
        copy.start()
    for m in range(3):
        w_local(m).start()
    group = x * 2 + yl
    kinds = []
    for step in range(1, 8):
        dx, dy = step // 2, step % 2
        kinds.append(
            rc(mod_ref, mod_all.at[group], MM + step - 1, MM + step - 1,
               x=(x + dx) % 4, yl=(yl + dy) % 2)
        )
    for copy in kinds:
        copy.start()
    mod_all[group] = mod_ref[...]
    eye_f[...] = eye(ff)
    eye_q[...] = eye(quarter)
    for copy in loads:
        copy.wait()

    def h_block(q, source):
        return ht_ref.at[q, :, tile(source, quarter)]

    def h_right(k):
        return rc(h_block(order(k), x), h_block(order(k), x), HR + k, HR + k, x=right)

    def h_left(k):
        return rc(h_block(order(k), x), h_block(order(k), x), HL + k, HL + k, x=left)

    def h_on_right(k):
        block = ht_ref.at[order(k), top, tile(left, quarter)]
        return rc(block, block, HFR + k, HFR + k, x=right)

    def h_on_left(k):
        block = ht_ref.at[order(k), low, tile(right, quarter)]
        return rc(block, block, HFL + k, HFL + k, x=left)

    def make_hidden(k, _):
        q = order(k)
        g = gate_v[tile(q, quarter), :].astype(F32)
        u = up_v[tile(q, quarter), :].astype(F32)
        hidden = (g * jax.nn.sigmoid(g) * u).astype(BF16)
        ht_ref[q, :, tile(x, quarter)] = dot_nt(eye_f[...], hidden).astype(BF16)
        h_right(k).start()
        h_left(k).start()
        return 0

    lax.fori_loop(0, 4, make_hidden, 0)

    def first_in(source):
        dst = first_dst(z, source)
        return rc(dst, dst, S1, S1 + source, x=right)

    def swap(e):
        block = s_block(z, e, c)
        return rc(block, block, YH, YH, yh=1 - yh)

    def ring(q, e, i, to):
        block = s_block(q, e, c)
        return rc(block, block, ZZ + i, ZZ + i, z=to)

    def share(k, e, core):
        block = s_block(order(k), e, core)
        return rc(block, block, CC + 2 * k + e, CC + 2 * k + e, c=1 - c)

    for source in range(4):
        first_in(source).wait_recv()
    swap(0).start()
    ring(z, 0, 0, up_z).start()
    ring(z, 0, 2, down_z).start()
    share(0, 0, c).start()
    w_copy(1).start()
    w_copy(2).start()

    def pass_hidden(k, _):
        q = order(k)
        a = h_block(q, left)
        rc(a, a, HR + k, HR + k, x=right).wait_recv()
        h_on_right(k).start()
        b = h_block(q, right)
        rc(b, b, HL + k, HL + k, x=left).wait_recv()
        h_on_left(k).start()
        return 0

    lax.fori_loop(0, 2, pass_hidden, 0)
    ring(down_z, 0, 0, up_z).wait_recv()
    ring(down_z, 0, 4, up_z).start()
    share(1, 0, c).start()
    ring(up_z, 0, 2, down_z).wait_recv()
    share(2, 0, c).start()
    swap(1).wait_recv()
    ring(z, 1, 1, up_z).start()
    ring(z, 1, 3, down_z).start()
    share(0, 1, c).start()
    lax.fori_loop(2, 4, pass_hidden, 0)
    ring(up_z, 1, 3, down_z).wait_recv()
    ring(up_z, 1, 5, down_z).start()
    share(2, 1, c).start()
    ring(down_z, 1, 1, up_z).wait_recv()
    share(1, 1, c).start()
    far = (z + 2) % 4
    ring(far, 0, 4, up_z).wait_recv()
    share(3, 0, c).start()
    ring(far, 1, 5, down_z).wait_recv()
    share(3, 1, c).start()

    for step in range(1, 8):
        dx, dy = step // 2, step % 2
        source = ((x + 4 - dx) % 4) * 2 + (yl + dy) % 2
        rc(mod_ref, mod_all.at[source], MM, MM + step - 1, x=right).wait_recv()
    for q in range(4):
        pieces = []
        for source in range(4):
            one = mod_all[source * 2 + yl]
            pieces += [one[2 * q : 2 * q + 1, :], one[2 * q + 1 : 2 * q + 2, :]]
        kind_ref[q] = jnp.concatenate(pieces, axis=1)
    everyone = mod_all[...].reshape(rows // 128 * 8, 128)
    factors = []
    for m in range(3):
        hits = (everyone == m).astype(F32)
        count = jnp.sum(jnp.sum(hits, axis=0, keepdims=True), axis=1, keepdims=True)
        factors.append(total / (3.0 * count))

    for m in range(3):
        w_local(m).wait()
        theirs = wv_ref.at[m, :, tile(1 - yl, half)]
        rc(theirs, theirs, WW + m, WW + m, yl=1 - yl).wait_recv()

    def hop(k, to_right):
        q = order(k)
        if to_right:
            return rc(part_ref.at[across, q, top, :], hop_left.at[k], TR + k, TR + k, x=right)
        return rc(part_ref.at[across, q, low, :], hop_right.at[k], TL + k, TL + k, x=left)

    def give(k, to_right, rows_at, base):
        q = order(k)
        if to_right:
            return rc(part_ref.at[right, q, rows_at, :], from_left.at[k, rows_at, :],
                      base + k, base + k, x=right)
        return rc(part_ref.at[left, q, rows_at, :], from_right.at[k, rows_at, :],
                  base + k, base + k, x=left)

    def gives(k, i):
        return give(k, i % 2 == 0, (low, top, top, low)[i], (DR1, DL1, DR2, DL2)[i])

    def relay(k):
        q = order(k)
        hop(k, True).wait_recv()
        part_ref[right, q, top, :] = (
            part_ref[right, q, top, :].astype(F32) + hop_left[k].astype(F32)
        ).astype(BF16)
        gives(k, 2).start()
        hop(k, False).wait_recv()
        part_ref[left, q, low, :] = (
            part_ref[left, q, low, :].astype(F32) + hop_right[k].astype(F32)
        ).astype(BF16)
        gives(k, 3).start()

    def share_in(k, e):
        share(k, e, 1 - c).wait_recv()

    def hidden_step(k, _):
        q = order(k)
        share_in(k, 0)
        share_in(k, 1)

        def pair(p, _):
            block = s_ref[q, tile(p, half), :]
            kind = kind_ref[q, :, tile(p, half)]
            got = dot_nt(wv_ref[0], block)
            for m in range(1, 3):
                got = jnp.where(kind == m, dot_nt(wv_ref[m], block), got)
            got = got.astype(BF16)
            part_ref[2 * p, q] = got[:, :quarter]
            part_ref[2 * p + 1, q] = got[:, quarter:]
            return 0

        lax.fori_loop(0, 2, pair, 0)
        hop(k, True).start()
        hop(k, False).start()
        gives(k, 0).start()
        gives(k, 1).start()

        @pl.when(k > 0)
        def _():
            relay(k - 1)

        return 0

    lax.fori_loop(0, 4, hidden_step, 0)

    def hidden_in(k, _):
        a = ht_ref.at[order(k), top, tile(across, quarter)]
        rc(a, a, HFR + k, HFR + k, x=right).wait_recv()
        b = ht_ref.at[order(k), low, tile(across, quarter)]
        rc(b, b, HFL + k, HFL + k, x=left).wait_recv()
        return 0

    lax.fori_loop(0, 4, hidden_in, 0)

    def weight_sum(m, side, dst):
        dst[...] = jnp.zeros(dst.shape, F32)

        def add(q, _):
            mark = (kind_ref[q] == m).astype(F32).astype(BF16)
            dst[...] += jnp.dot(
                ht_ref[q] * mark, s_ref[q, :, tile(side, half)], preferred_element_type=F32
            )
            return 0

        lax.fori_loop(0, 4, add, 0)

    def dw_copy(m):
        return rc(out_half.at[m], in_half.at[m], DW + m, DW + m, yl=1 - yl)

    def other_half(m, _):
        weight_sum(m, 1 - yl, acc_ref)
        out_half[m] = acc_ref[...].astype(BF16)
        dw_copy(m).start()

        @pl.when(m == 0)
        def _():
            relay(3)

        return 0

    lax.fori_loop(0, 3, other_half, 0)

    def own_half(m, _):
        weight_sum(m, yl, dw_ref.at[m])
        return 0

    lax.fori_loop(0, 3, own_half, 0)

    def finish(k, _):
        q = order(k)
        for i in range(4):
            gives(k, i).wait_recv()
        kind = kind_ref[q, :, tile(x, quarter)]
        scale = jnp.where(kind == 0, factors[0], jnp.where(kind == 1, factors[1], factors[2]))
        t = (
            part_ref[x, q].astype(F32) + from_left[k].astype(F32) + from_right[k].astype(F32)
        ) * scale
        high = t.astype(BF16)
        rest = (t - high.astype(F32)).astype(BF16)
        d = dot_nt(eye_q[...], high) + dot_nt(eye_q[...], rest)
        g = gate_v[tile(q, quarter), :].astype(F32)
        u = up_v[tile(q, quarter), :].astype(F32)
        s = jax.nn.sigmoid(g)
        ug_ref[tile(q, quarter), :] = (d * (g * s)).astype(BF16)
        gg_ref[tile(q, quarter), :] = (d * u * (s * (1.0 + g * (1.0 - s)))).astype(BF16)
        return 0

    lax.fori_loop(0, 4, finish, 0)
    for m in range(3):
        dw_copy(m).wait_recv()
        dw_ref[m] = (dw_ref[m] + in_half[m].astype(F32)) * factors[m]

    for q in range(4):
        @pl.when(jnp.logical_not(is_self(q)))
        def _():
            first_remote(q).wait_send()

    for copy in kinds:
        copy.wait_send()
    swap(0).wait_send()
    for q, e, i, to in (
        (z, 0, 0, up_z), (z, 1, 1, up_z), (z, 0, 2, down_z),
        (z, 1, 3, down_z), (down_z, 0, 4, up_z), (up_z, 1, 5, down_z),
    ):
        ring(q, e, i, to).wait_send()

    def drain(k, _):
        for copy in (h_right(k), h_left(k), h_on_right(k), h_on_left(k)):
            copy.wait_send()
        for copy in (share(k, 0, c), share(k, 1, c), hop(k, True), hop(k, False)):
            copy.wait_send()
        for i in range(4):
            gives(k, i).wait_send()
        return 0

    lax.fori_loop(0, 4, drain, 0)
    for m in range(3):
        w_copy(m).wait_send()
        dw_copy(m).wait_send()


def shards(modality, out_grad, gate_pre, up_pre, down_weight):
    rows, cols = out_grad.shape
    kinds, ff, half = down_weight.shape
    quarter = rows // 4
    cut = (ff // 2 + 15) // 16 * 16
    anywhere = pl.BlockSpec(memory_space=pl.ANY)
    vmem = pl.BlockSpec(memory_space=pltpu.VMEM)
    return pl.pallas_call(
        kernel,
        out_shape=(
            jax.ShapeDtypeStruct((kinds, ff, half), F32),
            jax.ShapeDtypeStruct((rows, ff), BF16),
            jax.ShapeDtypeStruct((rows, ff), BF16),
        ),
        in_specs=[vmem, anywhere, anywhere, anywhere, anywhere],
        out_specs=(vmem, vmem, vmem),
        scratch_shapes=[
            pltpu.VMEM((4, rows, 4 * cols), BF16),
            pltpu.VMEM((kinds, ff, 2 * half), BF16),
            pltpu.VMEM((4, ff, rows), BF16),
            pltpu.VMEM((4, 4, ff, quarter), BF16),
            pltpu.VMEM((4, ff, quarter), BF16),
            pltpu.VMEM((4, ff, quarter), BF16),
            pltpu.VMEM((4, cut, quarter), BF16),
            pltpu.VMEM((4, ff - cut, quarter), BF16),
            pltpu.VMEM((ff, half), F32),
            pltpu.VMEM((kinds, ff, half), BF16),
            pltpu.VMEM((kinds, ff, half), BF16),
            pltpu.VMEM((rows, ff), BF16),
            pltpu.VMEM((rows, ff), BF16),
            pltpu.VMEM((8, rows // 128, 128), jnp.int32),
            pltpu.VMEM((4, 1, rows), jnp.int32),
            pltpu.VMEM((ff, ff), BF16),
            pltpu.VMEM((quarter, quarter), BF16),
            pltpu.SemaphoreType.DMA((SEMS,)),
            pltpu.SemaphoreType.DMA((SEMS,)),
            pltpu.SemaphoreType.DMA((5,)),
        ],
        compiler_params=pltpu.CompilerParams(
            has_side_effects=True, vmem_limit_bytes=67_000_000
        ),
    )(modality.reshape(rows // 128, 128), out_grad, gate_pre, up_pre, down_weight)


def solution(mesh):
    torus = Mesh(mesh.devices.reshape(4, 2, 4, 2, 2), AXES)
    fsdp, tensor = ("x", "yl"), ("z", "yh", "c")
    in_specs = (
        P(fsdp),
        P(fsdp, tensor),
        P(fsdp, tensor),
        P(fsdp, tensor),
        P(None, tensor, fsdp),
    )
    out_specs = (P(None, tensor, fsdp), P(fsdp, tensor), P(fsdp, tensor))
    return jax.shard_map(
        shards, mesh=torus, in_specs=in_specs, out_specs=out_specs, check_vma=False
    )
```

```python
import jax
import jax.numpy as jnp
from jax import lax
from jax.experimental import pallas as pl
from jax.experimental.pallas import tpu as pltpu
from jax.sharding import Mesh
from jax.sharding import PartitionSpec as P

AXES = ("x", "yl", "z", "yh", "c")
MESH = pl.DeviceIdType.MESH
F32, BF16 = jnp.float32, jnp.bfloat16
S1, Z1, YH, UP0, UP1, DN0, DN1, FUP, FDN, CC = 0, 4, 8, 12, 16, 20, 24, 28, 32, 36
WW, MM, HR, HL, HFR, HFL = 68, 71, 78, 82, 86, 90
TR, TL, DR1, DL1, DR2, DL2, DW, SEMS = 94, 98, 102, 106, 110, 114, 118, 121


def dot_nt(a, b):
    return lax.dot_general(a, b, (((1,), (1,)), ((), ())), preferred_element_type=F32)


def kernel(
    mod_ref, og_ref, gate_ref, up_ref, w_ref, own_ref, theirs_ref, factor_ref, gg_ref, ug_ref,
    zin_ref, s_ref, wv_ref, ht_ref, part_ref, from_left, from_right, hop_left, hop_right,
    acc_ref, own_v, out_half, gate_v, up_v, mod_all, kind_ref,
    send, recv, local,
):
    x, yl, z, yh, c = (lax.axis_index(a) for a in AXES)
    ff, rows = gate_ref.shape
    quarter, cols = rows // 4, og_ref.shape[1]
    half = 2 * cols
    total = rows * 8
    cut = (ff // 2 + 15) // 16 * 16
    top, low = pl.ds(0, cut), pl.ds(cut, ff - cut)
    right, left, across = (x + 1) % 4, (x + 3) % 4, (x + 2) % 4
    up_z, down_z = (z + 1) % 4, (z + 3) % 4
    diagonal = x == z

    barrier = pltpu.get_barrier_semaphore()
    group_steps = [(s // 2, s % 2) for s in range(1, 8)]
    for dx, dy in group_steps:
        pl.semaphore_signal(
            barrier, inc=1, device_id={"x": (x + dx) % 4, "yl": (yl + dy) % 2}, device_id_type=MESH
        )
    for d in range(1, 4):
        pl.semaphore_signal(barrier, inc=1, device_id={"z": (z + d) % 4}, device_id_type=MESH)
    pl.semaphore_signal(barrier, inc=1, device_id={"yh": 1 - yh}, device_id_type=MESH)
    pl.semaphore_signal(barrier, inc=1, device_id={"c": 1 - c}, device_id_type=MESH)

    def rc(src, dst, si, ri, **where):
        return pltpu.make_async_remote_copy(
            src_ref=src, dst_ref=dst, send_sem=send.at[si], recv_sem=recv.at[ri],
            device_id=where, device_id_type=MESH,
        )

    def turn(i):
        return 3 * i + 3 * (i // 2) + 2 * (i // 3)

    def order(k):
        return (z + turn(k)) % 4

    def source(j):
        return (x + turn(j)) % 4

    def tile(i, n):
        return pl.ds(pl.multiple_of(i * n, n), n)

    def each(n, body, start=0):
        def step(i, _):
            body(i)
            return 0

        lax.fori_loop(start, n, step, 0)

    loads = [
        pltpu.make_async_copy(gate_ref, gate_v, local.at[0]),
        pltpu.make_async_copy(up_ref, up_v, local.at[1]),
    ]
    for copy in loads:
        copy.start()

    def w_copy(m):
        return rc(w_ref.at[m], wv_ref.at[m, :, tile(yl, half)], WW + m, WW + m, yl=1 - yl)

    def w_local(m):
        return pltpu.make_async_copy(w_ref.at[m], wv_ref.at[m, :, tile(yl, half)], local.at[2 + m])

    for m in range(3):
        w_local(m).start()
    group = x * 2 + yl
    mod_all[group] = mod_ref[...]
    for copy in loads:
        copy.wait()

    def make_hidden(k):
        q = order(k)
        g = gate_v[:, tile(q, quarter)].astype(F32)
        u = up_v[:, tile(q, quarter)].astype(F32)
        ht_ref[q, :, tile(x, quarter)] = (g * jax.nn.sigmoid(g) * u).astype(BF16)

    each(1, make_hidden)
    pl.semaphore_wait(barrier, 12)

    def s_first(q, src):
        return s_ref.at[q, tile(src, quarter), tile(yh * 2 + c, cols)]

    def along_z(d, direct):
        q = (z + d) % 4
        src = og_ref.at[tile(q, quarter), :]
        if direct:
            return rc(src, s_first(q, x), Z1 + d, S1 + x, z=q)
        return rc(src, zin_ref.at[d], Z1 + d, Z1 + d, z=q)

    def home():
        return rc(og_ref.at[tile(z, quarter), :], s_first(z, x), Z1, S1 + x, x=z)

    def along_x(d):
        return rc(zin_ref.at[d], s_first(z, x), S1 + d, S1 + x, x=(z + 4 - d) % 4)

    def passes(d):
        return (z + 4 - d) % 4 != x

    @pl.when(diagonal)
    def _():
        for d in (1, 3, 2):
            along_z(d, True).start()
        pltpu.make_async_copy(
            og_ref.at[tile(z, quarter), :], s_first(z, x), recv.at[S1 + x]
        ).start()

    @pl.when(jnp.logical_not(diagonal))
    def _():
        for d in (1, 3, 2):
            along_z(d, False).start()
        home().start()

    w_copy(0).start()

    def kinds_copy(i):
        dx, dy = group_steps[i]
        return rc(mod_ref, mod_all.at[group], MM + i, MM + i, x=(x + dx) % 4, yl=(yl + dy) % 2)

    for i in range(7):
        kinds_copy(i).start()

    def h_block(q, src):
        return ht_ref.at[q, :, tile(src, quarter)]

    def h_right(k):
        return rc(h_block(order(k), x), h_block(order(k), x), HR + k, HR + k, x=right)

    def h_left(k):
        return rc(h_block(order(k), x), h_block(order(k), x), HL + k, HL + k, x=left)

    def h_on_right(k):
        block = ht_ref.at[order(k), top, tile(left, quarter)]
        return rc(block, block, HFR + k, HFR + k, x=right)

    def h_on_left(k):
        block = ht_ref.at[order(k), low, tile(right, quarter)]
        return rc(block, block, HFL + k, HFL + k, x=left)

    def send_hidden(k):
        h_right(k).start()
        h_left(k).start()

    send_hidden(0)
    each(4, make_hidden, 1)
    acc_ref[...] = jnp.zeros(acc_ref.shape, F32)

    for d in (1, 3, 2):
        @pl.when(passes(d))
        def _():
            rc(zin_ref.at[d], zin_ref.at[d], Z1 + d, Z1 + d, z=z).wait_recv()
            along_x(d).start()

    each(4, send_hidden, 1)

    def piece(q, e, core, j):
        return s_ref.at[q, tile(source(j), quarter), tile(((yh + e) % 2) * 2 + core, cols)]

    def swap(e, j):
        return rc(piece(z, e, c, j), piece(z, e, c, j), YH + j, YH + j, yh=1 - yh)

    def ring(q, e, j, base, to):
        return rc(piece(q, e, c, j), piece(q, e, c, j), base + j, base + j, z=to)

    def share(k, e, j, core):
        i = CC + 8 * k + 4 * e + j
        return rc(piece(order(k), e, core, j), piece(order(k), e, core, j), i, i, c=1 - c)

    def spread_own(j):
        dst = s_first(z, source(j))
        rc(dst, dst, S1, S1 + source(j), x=right).wait_recv()
        swap(0, j).start()
        ring(z, 0, j, UP0, up_z).start()
        ring(z, 0, j, DN0, down_z).start()
        share(0, 0, j, c).start()

    each(4, spread_own)
    w_copy(1).start()
    w_copy(2).start()

    def pass_hidden(k):
        q = order(k)
        rc(h_block(q, left), h_block(q, left), HR + k, HR + k, x=right).wait_recv()
        h_on_right(k).start()
        rc(h_block(q, right), h_block(q, right), HL + k, HL + k, x=left).wait_recv()
        h_on_left(k).start()

    each(1, pass_hidden)

    def spread_other(j):
        swap(1, j).wait_recv()
        ring(z, 1, j, UP1, up_z).start()
        ring(z, 1, j, DN1, down_z).start()
        share(0, 1, j, c).start()
        ring(down_z, 0, j, UP0, up_z).wait_recv()
        ring(down_z, 0, j, FUP, up_z).start()
        share(1, 0, j, c).start()
        ring(up_z, 0, j, DN0, down_z).wait_recv()
        share(2, 0, j, c).start()

    each(4, spread_other)
    each(3, pass_hidden, 1)

    for i in range(7):
        dx, dy = group_steps[i]
        src = ((x + 4 - dx) % 4) * 2 + (yl + dy) % 2
        rc(mod_ref, mod_all.at[src], MM, MM + i, x=right).wait_recv()
    for q in range(4):
        pieces = []
        for src in range(4):
            one = mod_all[src * 2 + yl]
            pieces += [one[2 * q : 2 * q + 1, :], one[2 * q + 1 : 2 * q + 2, :]]
        kind_ref[q] = jnp.concatenate(pieces, axis=1)
    everyone = mod_all[...].reshape(rows // 128 * 8, 128)
    factors = []
    for m in range(3):
        hits = (everyone == m).astype(F32)
        count = jnp.sum(jnp.sum(hits, axis=0, keepdims=True), axis=1, keepdims=True)
        factors.append(total / (3.0 * count))
        factor_ref[m : m + 1, :] = jnp.broadcast_to(factors[m], (1, 128))

    def block_in(k):
        def one(i):
            share(k, i // 4, i % 4, 1 - c).wait_recv()

        each(8, one)

    def hidden_in(k):
        q = order(k)
        a = ht_ref.at[q, top, tile(across, quarter)]
        rc(a, a, HFR + k, HFR + k, x=right).wait_recv()
        b = ht_ref.at[q, low, tile(across, quarter)]
        rc(b, b, HFL + k, HFL + k, x=left).wait_recv()

    def marked(q, m):
        return ht_ref[q] * (kind_ref[q] == m).astype(F32).astype(BF16)

    def add_quarter(k):
        q = order(k)
        block_in(k)
        hidden_in(k)

        def one(m):
            acc_ref[m] += jnp.dot(marked(q, m), s_ref[q], preferred_element_type=F32)

        each(3, one)

    def spread_near(j):
        ring(up_z, 1, j, DN1, down_z).wait_recv()
        ring(up_z, 1, j, FDN, down_z).start()
        share(2, 1, j, c).start()
        ring(down_z, 1, j, UP1, up_z).wait_recv()
        share(1, 1, j, c).start()

    far = (z + 2) % 4

    def spread_far(j):
        ring(far, 0, j, FUP, up_z).wait_recv()
        share(3, 0, j, c).start()
        ring(far, 1, j, FDN, down_z).wait_recv()
        share(3, 1, j, c).start()

    each(4, spread_near)
    each(4, pass_hidden, 3)
    each(2, add_quarter)
    each(4, spread_far)
    each(3, add_quarter, 2)
    for m in range(3):
        w_local(m).wait()
        theirs = wv_ref.at[m, :, tile(1 - yl, half)]
        rc(theirs, theirs, WW + m, WW + m, yl=1 - yl).wait_recv()

    def hop(k, to_right):
        q = order(k)
        if to_right:
            return rc(part_ref.at[across, q, top, :], hop_left.at[k], TR + k, TR + k, x=right)
        return rc(part_ref.at[across, q, low, :], hop_right.at[k], TL + k, TL + k, x=left)

    def give(k, to_right, rows_at, base):
        q = order(k)
        if to_right:
            return rc(part_ref.at[right, q, rows_at, :], from_left.at[k, rows_at, :],
                      base + k, base + k, x=right)
        return rc(part_ref.at[left, q, rows_at, :], from_right.at[k, rows_at, :],
                  base + k, base + k, x=left)

    def gives(k, i):
        return give(k, i % 2 == 0, (low, top, top, low)[i], (DR1, DL1, DR2, DL2)[i])

    def relay(k):
        q = order(k)
        hop(k, True).wait_recv()
        part_ref[right, q, top, :] = (
            part_ref[right, q, top, :].astype(F32) + hop_left[k].astype(F32)
        ).astype(BF16)
        gives(k, 2).start()
        hop(k, False).wait_recv()
        part_ref[left, q, low, :] = (
            part_ref[left, q, low, :].astype(F32) + hop_right[k].astype(F32)
        ).astype(BF16)
        gives(k, 3).start()

    def d_hidden(k):
        q = order(k)

        def pair(p):
            block = s_ref[q, tile(p, half), :]
            kind = kind_ref[q, :, tile(p, half)]
            got = dot_nt(wv_ref[0], block)
            for m in range(1, 3):
                got = jnp.where(kind == m, dot_nt(wv_ref[m], block), got)
            got = got.astype(BF16)
            part_ref[2 * p, q] = got[:, :quarter]
            part_ref[2 * p + 1, q] = got[:, quarter:]

        each(2, pair)
        hop(k, True).start()
        hop(k, False).start()
        gives(k, 0).start()
        gives(k, 1).start()

    def dw_copy(m):
        return rc(out_half.at[m], theirs_ref.at[m], DW + m, DW + m, yl=1 - yl)

    def own_out(m):
        return pltpu.make_async_copy(own_v.at[m], own_ref.at[m], local.at[5 + m])

    def last_sum(m, side):
        q = order(3)
        at = tile(side, half)
        return acc_ref[m, :, at] + jnp.dot(
            marked(q, m), s_ref[q, :, at], preferred_element_type=F32
        )

    def other_half(m):
        out_half[m] = last_sum(m, 1 - yl).astype(BF16)
        dw_copy(m).start()

    def own_half(m):
        own_v[m] = last_sum(m, yl).astype(BF16)
        own_out(m).start()

    d_hidden(0)
    block_in(3)
    hidden_in(3)
    each(3, other_half)

    def more_d_hidden(k):
        d_hidden(k)
        relay(k - 1)

    each(4, more_d_hidden, 1)
    each(3, own_half)
    relay(3)

    def grads_out(k):
        at = tile(order(k), quarter)
        return (
            pltpu.make_async_copy(up_v.at[:, at], ug_ref.at[:, at], local.at[8 + k]),
            pltpu.make_async_copy(gate_v.at[:, at], gg_ref.at[:, at], local.at[12 + k]),
        )

    def finish(k):
        q = order(k)
        for i in range(4):
            gives(k, i).wait_recv()
        kind = kind_ref[q, :, tile(x, quarter)]
        scale = jnp.where(kind == 0, factors[0], jnp.where(kind == 1, factors[1], factors[2]))
        t = scale * (
            part_ref[x, q].astype(F32) + from_left[k].astype(F32) + from_right[k].astype(F32)
        )
        g = gate_v[:, tile(q, quarter)].astype(F32)
        u = up_v[:, tile(q, quarter)].astype(F32)
        s = jax.nn.sigmoid(g)
        up_v[:, tile(q, quarter)] = (t * (g * s)).astype(BF16)
        gate_v[:, tile(q, quarter)] = (t * u * (s * (1.0 + g * (1.0 - s)))).astype(BF16)
        for copy in grads_out(k):
            copy.start()

    each(4, finish)
    for m in range(3):
        own_out(m).wait()
        dw_copy(m).wait_recv()

    @pl.when(diagonal)
    def _():
        for d in range(1, 4):
            along_z(d, True).wait_send()

    @pl.when(jnp.logical_not(diagonal))
    def _():
        for d in range(1, 4):
            along_z(d, False).wait_send()
        home().wait_send()

    for d in range(1, 4):
        @pl.when(passes(d))
        def _():
            along_x(d).wait_send()

    for i in range(7):
        kinds_copy(i).wait_send()

    def drain(k):
        for copy in grads_out(k):
            copy.wait()
        swap(0, k).wait_send()
        for q, e, base, to in (
            (z, 0, UP0, up_z), (z, 1, UP1, up_z), (z, 0, DN0, down_z),
            (z, 1, DN1, down_z), (down_z, 0, FUP, up_z), (up_z, 1, FDN, down_z),
        ):
            ring(q, e, k, base, to).wait_send()
        for copy in (h_right(k), h_left(k), h_on_right(k), h_on_left(k)):
            copy.wait_send()
        for i in range(8):
            share(k, i // 4, i % 4, c).wait_send()
        for copy in (hop(k, True), hop(k, False)):
            copy.wait_send()
        for i in range(4):
            gives(k, i).wait_send()

    each(4, drain)
    for m in range(3):
        w_copy(m).wait_send()
        dw_copy(m).wait_send()


def shards(modality, out_grad, gate_pre, up_pre, down_weight):
    rows, cols = out_grad.shape
    kinds, ff, half = down_weight.shape
    quarter = rows // 4
    cut = (ff // 2 + 15) // 16 * 16
    anywhere = pl.BlockSpec(memory_space=pl.ANY)
    vmem = pl.BlockSpec(memory_space=pltpu.VMEM)
    own, theirs, factor, gate_grad, up_grad = pl.pallas_call(
        kernel,
        out_shape=(
            jax.ShapeDtypeStruct((kinds, ff, half), BF16),
            jax.ShapeDtypeStruct((kinds, ff, half), BF16),
            jax.ShapeDtypeStruct((kinds, 128), F32),
            jax.ShapeDtypeStruct((ff, rows), BF16),
            jax.ShapeDtypeStruct((ff, rows), BF16),
        ),
        in_specs=[vmem, anywhere, anywhere, anywhere, anywhere],
        out_specs=(anywhere, anywhere, vmem, anywhere, anywhere),
        scratch_shapes=[
            pltpu.VMEM((4, quarter, cols), BF16),
            pltpu.VMEM((4, rows, 4 * cols), BF16),
            pltpu.VMEM((kinds, ff, 2 * half), BF16),
            pltpu.VMEM((4, ff, rows), BF16),
            pltpu.VMEM((4, 4, ff, quarter), BF16),
            pltpu.VMEM((4, ff, quarter), BF16),
            pltpu.VMEM((4, ff, quarter), BF16),
            pltpu.VMEM((4, cut, quarter), BF16),
            pltpu.VMEM((4, ff - cut, quarter), BF16),
            pltpu.VMEM((kinds, ff, 2 * half), F32),
            pltpu.VMEM((kinds, ff, half), BF16),
            pltpu.VMEM((kinds, ff, half), BF16),
            pltpu.VMEM((ff, rows), BF16),
            pltpu.VMEM((ff, rows), BF16),
            pltpu.VMEM((8, rows // 128, 128), jnp.int32),
            pltpu.VMEM((4, 1, rows), jnp.int32),
            pltpu.SemaphoreType.DMA((SEMS,)),
            pltpu.SemaphoreType.DMA((SEMS,)),
            pltpu.SemaphoreType.DMA((16,)),
        ],
        compiler_params=pltpu.CompilerParams(
            collective_id=0, has_side_effects=True, vmem_limit_bytes=67_000_000
        ),
    )(modality.reshape(rows // 128, 128), out_grad, gate_pre.T, up_pre.T, down_weight)
    down_grad = (own.astype(F32) + theirs.astype(F32)) * factor[:, :1, None]
    return down_grad, gate_grad.T, up_grad.T


def solution(mesh):
    torus = Mesh(mesh.devices.reshape(4, 2, 4, 2, 2), AXES)
    fsdp, tensor = ("x", "yl"), ("z", "yh", "c")
    in_specs = (
        P(fsdp),
        P(fsdp, tensor),
        P(fsdp, tensor),
        P(fsdp, tensor),
        P(None, tensor, fsdp),
    )
    out_specs = (P(None, tensor, fsdp), P(fsdp, tensor), P(fsdp, tensor))
    return jax.shard_map(
        shards, mesh=torus, in_specs=in_specs, out_specs=out_specs, check_vma=False
    )
```

```python
import jax
import jax.numpy as jnp
from jax import lax
from jax.experimental import pallas as pl
from jax.experimental.pallas import tpu as pltpu
from jax.sharding import Mesh
from jax.sharding import PartitionSpec as P

AXES = ("x", "yl", "z", "yh", "c")
MESH = pl.DeviceIdType.MESH
F32, BF16 = jnp.float32, jnp.bfloat16
S1, Z1, YH, UP0, UP1, DN0, DN1, FUP, FDN, CC = 0, 4, 8, 12, 16, 20, 24, 28, 32, 36
WW, MM, HR, HL, HFR, HFL = 68, 74, 81, 85, 89, 93
TR, TL, DR1, DL1, DR2, DL2, DW, SEMS = 97, 101, 105, 109, 113, 117, 121, 124


def dot_nt(a, b):
    return lax.dot_general(a, b, (((1,), (1,)), ((), ())), preferred_element_type=F32)


def kernel(
    mod_ref, og_ref, gate_ref, up_ref, w_ref, own_ref, theirs_ref, factor_ref, gg_ref, ug_ref,
    zin_ref, s_ref, wv_ref, ht_ref, part_ref, from_left, from_right, hop_left, hop_right,
    acc_ref, dw_ref, early_ref, out_half, own_v, gate_v, up_v, mod_all, kind_ref,
    send, recv, local,
):
    x, yl, z, yh, c = (lax.axis_index(a) for a in AXES)
    ff, rows = gate_ref.shape
    quarter, cols = rows // 4, og_ref.shape[1]
    half = 2 * cols
    total = rows * 8
    cut = (ff // 2 + 15) // 16 * 16
    top, low = pl.ds(0, cut), pl.ds(cut, ff - cut)
    right, left, across = (x + 1) % 4, (x + 3) % 4, (x + 2) % 4
    up_z, down_z = (z + 1) % 4, (z + 3) % 4
    diagonal = x == z

    barrier = pltpu.get_barrier_semaphore()
    group_steps = [(s // 2, s % 2) for s in range(1, 8)]
    for dx, dy in group_steps:
        pl.semaphore_signal(
            barrier, inc=1, device_id={"x": (x + dx) % 4, "yl": (yl + dy) % 2}, device_id_type=MESH
        )
    for d in range(1, 4):
        pl.semaphore_signal(barrier, inc=1, device_id={"z": (z + d) % 4}, device_id_type=MESH)
    pl.semaphore_signal(barrier, inc=1, device_id={"yh": 1 - yh}, device_id_type=MESH)
    pl.semaphore_signal(barrier, inc=1, device_id={"c": 1 - c}, device_id_type=MESH)

    def rc(src, dst, si, ri, **where):
        return pltpu.make_async_remote_copy(
            src_ref=src, dst_ref=dst, send_sem=send.at[si], recv_sem=recv.at[ri],
            device_id=where, device_id_type=MESH,
        )

    def turn(i):
        return 3 * i + 3 * (i // 2) + 2 * (i // 3)

    def order(k):
        return (z + turn(k)) % 4

    def source(j):
        return (x + turn(j)) % 4

    def tile(i, n):
        return pl.ds(pl.multiple_of(i * n, n), n)

    def each(n, body, start=0):
        def step(i, _):
            body(i)
            return 0

        lax.fori_loop(start, n, step, 0)

    loads = [
        pltpu.make_async_copy(gate_ref, gate_v, local.at[0]),
        pltpu.make_async_copy(up_ref, up_v, local.at[1]),
    ]
    group = x * 2 + yl
    kinds_in = pltpu.make_async_copy(mod_ref, mod_all.at[group], local.at[5])
    kinds_in.start()
    for copy in loads:
        copy.start()

    def w_piece(m, i, side):
        return wv_ref.at[m, (top, low)[i], tile(side, half)]

    def w_copy(m, i):
        src = w_ref.at[m, (top, low)[i], :]
        return rc(src, w_piece(m, i, yl), WW + 2 * m + i, WW + 2 * m + i, yl=1 - yl)

    def w_local(m):
        return pltpu.make_async_copy(w_ref.at[m], wv_ref.at[m, :, tile(yl, half)], local.at[2 + m])

    for m in range(3):
        w_local(m).start()

    def make_hidden(k):
        q = order(k)
        g = gate_v[:, tile(q, quarter)].astype(F32)
        u = up_v[:, tile(q, quarter)].astype(F32)
        ht_ref[q, :, tile(x, quarter)] = (g * jax.nn.sigmoid(g) * u).astype(BF16)

    pl.semaphore_wait(barrier, 12)

    def s_first(q, src):
        return s_ref.at[q, tile(src, quarter), tile(yh * 2 + c, cols)]

    def along_z(d, direct):
        q = (z + d) % 4
        src = og_ref.at[tile(q, quarter), :]
        if direct:
            return rc(src, s_first(q, x), Z1 + d, S1 + x, z=q)
        return rc(src, zin_ref.at[d], Z1 + d, Z1 + d, z=q)

    def home():
        return rc(og_ref.at[tile(z, quarter), :], s_first(z, x), Z1, S1 + x, x=z)

    def along_x(d):
        return rc(zin_ref.at[d], s_first(z, x), S1 + d, S1 + x, x=(z + 4 - d) % 4)

    def passes(d):
        return (z + 4 - d) % 4 != x

    @pl.when(diagonal)
    def _():
        for d in (1, 3, 2):
            along_z(d, True).start()
        pltpu.make_async_copy(
            og_ref.at[tile(z, quarter), :], s_first(z, x), recv.at[S1 + x]
        ).start()

    @pl.when(jnp.logical_not(diagonal))
    def _():
        for d in (1, 3, 2):
            along_z(d, False).start()
        home().start()

    w_copy(0, 0).start()
    w_copy(0, 1).start()

    def kinds_copy(i):
        dx, dy = group_steps[i]
        return rc(mod_ref, mod_all.at[group], MM + i, MM + i, x=(x + dx) % 4, yl=(yl + dy) % 2)

    def h_block(q, src):
        return ht_ref.at[q, :, tile(src, quarter)]

    def h_right(k):
        return rc(h_block(order(k), x), h_block(order(k), x), HR + k, HR + k, x=right)

    def h_left(k):
        return rc(h_block(order(k), x), h_block(order(k), x), HL + k, HL + k, x=left)

    def h_on_right(k):
        block = ht_ref.at[order(k), top, tile(left, quarter)]
        return rc(block, block, HFR + k, HFR + k, x=right)

    def h_on_left(k):
        block = ht_ref.at[order(k), low, tile(right, quarter)]
        return rc(block, block, HFL + k, HFL + k, x=left)

    def send_hidden(k):
        h_right(k).start()
        h_left(k).start()

    for copy in loads:
        copy.wait()
    each(1, make_hidden)
    send_hidden(0)
    for i in range(7):
        kinds_copy(i).start()
    each(4, make_hidden, 1)

    for d in (1, 3, 2):
        @pl.when(passes(d))
        def _():
            rc(zin_ref.at[d], zin_ref.at[d], Z1 + d, Z1 + d, z=z).wait_recv()
            along_x(d).start()

    send_hidden(1)
    acc_ref[...] = jnp.zeros(acc_ref.shape, F32)
    dw_ref[...] = jnp.zeros(dw_ref.shape, F32)

    def piece(q, e, core, j):
        return s_ref.at[q, tile(source(j), quarter), tile(((yh + e) % 2) * 2 + core, cols)]

    def swap(e, j):
        return rc(piece(z, e, c, j), piece(z, e, c, j), YH + j, YH + j, yh=1 - yh)

    def ring(q, e, j, base, to):
        return rc(piece(q, e, c, j), piece(q, e, c, j), base + j, base + j, z=to)

    def share(k, e, j, core):
        i = CC + 8 * k + 4 * e + j
        return rc(piece(order(k), e, core, j), piece(order(k), e, core, j), i, i, c=1 - c)

    def spread_own(j):
        dst = s_first(z, source(j))
        rc(dst, dst, S1, S1 + source(j), x=right).wait_recv()
        swap(0, j).start()
        ring(z, 0, j, UP0, up_z).start()
        ring(z, 0, j, DN0, down_z).start()
        share(0, 0, j, c).start()

    each(4, spread_own)
    w_copy(1, 0).start()
    w_copy(1, 1).start()
    w_copy(2, 0).start()
    w_copy(2, 1).start()

    def pass_hidden(k):
        q = order(k)
        rc(h_block(q, left), h_block(q, left), HR + k, HR + k, x=right).wait_recv()
        h_on_right(k).start()
        rc(h_block(q, right), h_block(q, right), HL + k, HL + k, x=left).wait_recv()
        h_on_left(k).start()

    pass_hidden(0)
    send_hidden(2)

    def spread_other(j):
        swap(1, j).wait_recv()
        ring(z, 1, j, UP1, up_z).start()
        ring(z, 1, j, DN1, down_z).start()
        share(0, 1, j, c).start()
        ring(down_z, 0, j, UP0, up_z).wait_recv()
        ring(down_z, 0, j, FUP, up_z).start()
        share(1, 0, j, c).start()
        ring(up_z, 0, j, DN0, down_z).wait_recv()
        share(2, 0, j, c).start()

    each(4, spread_other)
    pass_hidden(1)
    send_hidden(3)

    kinds_in.wait()
    for i in range(7):
        dx, dy = group_steps[i]
        src = ((x + 4 - dx) % 4) * 2 + (yl + dy) % 2
        rc(mod_ref, mod_all.at[src], MM, MM + i, x=right).wait_recv()
    for q in range(4):
        pieces = []
        for src in range(4):
            one = mod_all[src * 2 + yl]
            pieces += [one[2 * q : 2 * q + 1, :], one[2 * q + 1 : 2 * q + 2, :]]
        kind_ref[q] = jnp.concatenate(pieces, axis=1)
    everyone = mod_all[...].reshape(rows // 128 * 8, 128)
    factors = []
    for m in range(3):
        hits = (everyone == m).astype(F32)
        count = jnp.sum(jnp.sum(hits, axis=0, keepdims=True), axis=1, keepdims=True)
        factors.append(total / (3.0 * count))
        factor_ref[m : m + 1, :] = jnp.broadcast_to(factors[m], (1, 128))

    def block_in(k):
        def one(i):
            share(k, i // 4, i % 4, 1 - c).wait_recv()

        each(8, one)

    def hidden_in(k):
        q = order(k)
        a = ht_ref.at[q, top, tile(across, quarter)]
        rc(a, a, HFR + k, HFR + k, x=right).wait_recv()
        b = ht_ref.at[q, low, tile(across, quarter)]
        rc(b, b, HFL + k, HFL + k, x=left).wait_recv()

    def marked(q, m):
        return ht_ref[q] * (kind_ref[q] == m).astype(F32).astype(BF16)

    def add_quarter(k):
        q = order(k)
        block_in(k)
        hidden_in(k)

        def one(m):
            rows_marked = marked(q, m)
            for ref, side in ((acc_ref, 1 - yl), (dw_ref, yl)):
                ref[m] += jnp.dot(
                    rows_marked, s_ref[q, :, tile(side, half)], preferred_element_type=F32
                )

        each(3, one)

    def spread_near(j):
        ring(up_z, 1, j, DN1, down_z).wait_recv()
        ring(up_z, 1, j, FDN, down_z).start()
        share(2, 1, j, c).start()
        ring(down_z, 1, j, UP1, up_z).wait_recv()
        share(1, 1, j, c).start()

    far = (z + 2) % 4

    def spread_far(j):
        ring(far, 0, j, FUP, up_z).wait_recv()
        share(3, 0, j, c).start()
        ring(far, 1, j, FDN, down_z).wait_recv()
        share(3, 1, j, c).start()

    def two_blocks(p):
        return (x + 2 + p) % 4, (x + 1 + 3 * p) % 4

    def d_hidden_part(q, p, at):
        one, two = two_blocks(p)
        block = jnp.concatenate(
            [s_ref[q, tile(one, quarter), at], s_ref[q, tile(two, quarter), at]], axis=0
        )
        kind = jnp.concatenate(
            [kind_ref[q, :, tile(one, quarter)], kind_ref[q, :, tile(two, quarter)]], axis=1
        )
        got = dot_nt(wv_ref[0, :, at], block)
        for m in range(1, 3):
            got = jnp.where(kind == m, dot_nt(wv_ref[m, :, at], block), got)
        return got

    def early(p):
        early_ref[p] = d_hidden_part(z, p, tile(yl, half))

    add_quarter(0)
    each(4, spread_near)
    for m in range(3):
        w_local(m).wait()
    each(2, early)
    pass_hidden(2)
    add_quarter(1)
    each(4, spread_far)
    pass_hidden(3)
    add_quarter(2)
    for m in range(3):
        for i in range(2):
            theirs = w_piece(m, i, 1 - yl)
            rc(theirs, theirs, WW + 2 * m + i, WW + 2 * m + i, yl=1 - yl).wait_recv()

    def hop(k, to_right):
        q = order(k)
        if to_right:
            return rc(part_ref.at[across, q, top, :], hop_left.at[k], TR + k, TR + k, x=right)
        return rc(part_ref.at[across, q, low, :], hop_right.at[k], TL + k, TL + k, x=left)

    def give(k, to_right, rows_at, base):
        q = order(k)
        if to_right:
            return rc(part_ref.at[right, q, rows_at, :], from_left.at[k, rows_at, :],
                      base + k, base + k, x=right)
        return rc(part_ref.at[left, q, rows_at, :], from_right.at[k, rows_at, :],
                  base + k, base + k, x=left)

    def gives(k, i):
        return give(k, i % 2 == 0, (low, top, top, low)[i], (DR1, DL1, DR2, DL2)[i])

    def relay(k):
        q = order(k)
        hop(k, True).wait_recv()
        part_ref[right, q, top, :] = (
            part_ref[right, q, top, :].astype(F32) + hop_left[k].astype(F32)
        ).astype(BF16)
        gives(k, 2).start()
        hop(k, False).wait_recv()
        part_ref[left, q, low, :] = (
            part_ref[left, q, low, :].astype(F32) + hop_right[k].astype(F32)
        ).astype(BF16)
        gives(k, 3).start()

    def keep(q, p, got):
        got = got.astype(BF16)
        one, two = two_blocks(p)
        part_ref[one, q] = got[:, :quarter]
        part_ref[two, q] = got[:, quarter:]

    def send_first(k):
        hop(k, True).start()
        hop(k, False).start()
        gives(k, 0).start()

    def first_pair(p):
        keep(z, p, early_ref[p] + d_hidden_part(z, p, tile(1 - yl, half)))

        @pl.when(p == 0)
        def _():
            send_first(0)

    def d_hidden(k):
        q = order(k)

        def pair(p):
            keep(q, p, d_hidden_part(q, p, slice(None)))

            @pl.when(p == 0)
            def _():
                send_first(k)
                relay(k - 1)

        each(2, pair)
        gives(k, 1).start()

    def dw_copy(m):
        return rc(out_half.at[m], theirs_ref.at[m], DW + m, DW + m, yl=1 - yl)

    def last_sum(ref, m, side):
        q = order(3)
        return ref[m] + jnp.dot(
            marked(q, m), s_ref[q, :, tile(side, half)], preferred_element_type=F32
        )

    def own_out(m):
        return pltpu.make_async_copy(own_v.at[m], own_ref.at[m], local.at[6 + m])

    def grads_out(k):
        at = tile(order(k), quarter)
        return (
            pltpu.make_async_copy(up_v.at[:, at], ug_ref.at[:, at], local.at[9 + k]),
            pltpu.make_async_copy(gate_v.at[:, at], gg_ref.at[:, at], local.at[13 + k]),
        )

    def other_half(m):
        out_half[m] = last_sum(acc_ref, m, 1 - yl).astype(BF16)
        dw_copy(m).start()

    def own_half(m):
        own_v[m] = last_sum(dw_ref, m, yl).astype(BF16)
        own_out(m).start()

    block_in(3)
    hidden_in(3)
    other_half(0)
    each(2, first_pair)
    gives(0, 1).start()

    def steady(k):
        @pl.when(k < 3)
        def _():
            other_half(k)

        d_hidden(k)

    each(4, steady, 1)
    each(1, own_half)
    relay(3)
    each(3, own_half, 1)

    def finish(k):
        q = order(k)
        for i in range(4):
            gives(k, i).wait_recv()
        kind = kind_ref[q, :, tile(x, quarter)]
        scale = jnp.where(kind == 0, factors[0], jnp.where(kind == 1, factors[1], factors[2]))
        t = scale * (
            part_ref[x, q].astype(F32) + from_left[k].astype(F32) + from_right[k].astype(F32)
        )
        g = gate_v[:, tile(q, quarter)].astype(F32)
        u = up_v[:, tile(q, quarter)].astype(F32)
        s = jax.nn.sigmoid(g)
        up_v[:, tile(q, quarter)] = (t * (g * s)).astype(BF16)
        gate_v[:, tile(q, quarter)] = (t * u * (s * (1.0 + g * (1.0 - s)))).astype(BF16)
        for copy in grads_out(k):
            copy.start()

    each(4, finish)
    for m in range(3):
        own_out(m).wait()
        dw_copy(m).wait_recv()

    @pl.when(diagonal)
    def _():
        for d in range(1, 4):
            along_z(d, True).wait_send()

    @pl.when(jnp.logical_not(diagonal))
    def _():
        for d in range(1, 4):
            along_z(d, False).wait_send()
        home().wait_send()

    for d in range(1, 4):
        @pl.when(passes(d))
        def _():
            along_x(d).wait_send()

    for i in range(7):
        kinds_copy(i).wait_send()

    def drain(k):
        for copy in grads_out(k):
            copy.wait()
        swap(0, k).wait_send()
        for q, e, base, to in (
            (z, 0, UP0, up_z), (z, 1, UP1, up_z), (z, 0, DN0, down_z),
            (z, 1, DN1, down_z), (down_z, 0, FUP, up_z), (up_z, 1, FDN, down_z),
        ):
            ring(q, e, k, base, to).wait_send()
        for copy in (h_right(k), h_left(k), h_on_right(k), h_on_left(k)):
            copy.wait_send()
        for i in range(8):
            share(k, i // 4, i % 4, c).wait_send()
        for copy in (hop(k, True), hop(k, False)):
            copy.wait_send()
        for i in range(4):
            gives(k, i).wait_send()

    each(4, drain)
    for m in range(3):
        w_copy(m, 0).wait_send()
        w_copy(m, 1).wait_send()
        dw_copy(m).wait_send()


def store(
    own_ref, theirs_ref, factor_ref, gg_ref, ug_ref, dw_out, gg_out, ug_out,
    own_v, theirs_v, dw_v, gg_v, ug_v, come, go,
):
    ff = gg_ref.shape[0]
    cut = (ff // 2 + 15) // 16 * 16
    parts = [(m, at) for m in range(3) for at in (pl.ds(0, cut), pl.ds(cut, ff - cut))]
    copy = pltpu.make_async_copy
    grads_in = [copy(gg_ref, gg_v, come.at[0]), copy(ug_ref, ug_v, come.at[1])]
    grads_go = [copy(gg_v, gg_out, go.at[0]), copy(ug_v, ug_out, go.at[1])]
    sums_in = [
        (
            copy(own_ref.at[m, at, :], own_v.at[m, at, :], come.at[2 + 2 * i]),
            copy(theirs_ref.at[m, at, :], theirs_v.at[m, at, :], come.at[3 + 2 * i]),
        )
        for i, (m, at) in enumerate(parts)
    ]
    sums_go = [
        copy(dw_v.at[m, at, :], dw_out.at[m, at, :], go.at[2 + i]) for i, (m, at) in enumerate(parts)
    ]
    for one in grads_in:
        one.start()
    for pair in sums_in:
        for one in pair:
            one.start()
    for i in range(2):
        grads_in[i].wait()
        grads_go[i].start()
    for i, (m, at) in enumerate(parts):
        for one in sums_in[i]:
            one.wait()
        dw_v[m, at, :] = (own_v[m, at, :].astype(F32) + theirs_v[m, at, :].astype(F32)) * (
            factor_ref[m : m + 1, :1]
        )
        sums_go[i].start()
    for one in grads_go + sums_go:
        one.wait()


def shards(modality, out_grad, gate_pre, up_pre, down_weight):
    rows, cols = out_grad.shape
    kinds, ff, half = down_weight.shape
    quarter = rows // 4
    cut = (ff // 2 + 15) // 16 * 16
    hbm = pl.BlockSpec(memory_space=pltpu.HBM)
    vmem = pl.BlockSpec(memory_space=pltpu.VMEM)
    grad_shapes = (jax.ShapeDtypeStruct((ff, rows), BF16),) * 2
    shapes = (
        jax.ShapeDtypeStruct((kinds, ff, half), BF16),
        jax.ShapeDtypeStruct((kinds, ff, half), BF16),
        jax.ShapeDtypeStruct((kinds, 128), F32),
        *grad_shapes,
    )
    results = pl.pallas_call(
        kernel,
        out_shape=shapes,
        in_specs=[hbm] * 5,
        out_specs=(hbm, hbm, vmem, hbm, hbm),
        scratch_shapes=[
            pltpu.VMEM((4, quarter, cols), BF16),
            pltpu.VMEM((4, rows, 4 * cols), BF16),
            pltpu.VMEM((kinds, ff, 2 * half), BF16),
            pltpu.VMEM((4, ff, rows), BF16),
            pltpu.VMEM((4, 4, ff, quarter), BF16),
            pltpu.VMEM((4, ff, quarter), BF16),
            pltpu.VMEM((4, ff, quarter), BF16),
            pltpu.VMEM((4, cut, quarter), BF16),
            pltpu.VMEM((4, ff - cut, quarter), BF16),
            pltpu.VMEM((kinds, ff, half), F32),
            pltpu.VMEM((kinds, ff, half), F32),
            pltpu.VMEM((2, ff, half), F32),
            pltpu.VMEM((kinds, ff, half), BF16),
            pltpu.VMEM((kinds, ff, half), BF16),
            pltpu.VMEM((ff, rows), BF16),
            pltpu.VMEM((ff, rows), BF16),
            pltpu.VMEM((8, rows // 128, 128), jnp.int32),
            pltpu.VMEM((4, 1, rows), jnp.int32),
            pltpu.SemaphoreType.DMA((SEMS,)),
            pltpu.SemaphoreType.DMA((SEMS,)),
            pltpu.SemaphoreType.DMA((17,)),
        ],
        compiler_params=pltpu.CompilerParams(
            collective_id=0, has_side_effects=True, vmem_limit_bytes=60_000_000
        ),
    )(modality.reshape(rows // 128, 128), out_grad, gate_pre.T, up_pre.T, down_weight)
    down_grad, gate_grad, up_grad = pl.pallas_call(
        store,
        out_shape=(jax.ShapeDtypeStruct((kinds, ff, half), F32), *grad_shapes),
        in_specs=[hbm, hbm, vmem, hbm, hbm],
        out_specs=(hbm, hbm, hbm),
        scratch_shapes=[
            pltpu.VMEM((kinds, ff, half), BF16),
            pltpu.VMEM((kinds, ff, half), BF16),
            pltpu.VMEM((kinds, ff, half), F32),
            pltpu.VMEM((ff, rows), BF16),
            pltpu.VMEM((ff, rows), BF16),
            pltpu.SemaphoreType.DMA((14,)),
            pltpu.SemaphoreType.DMA((8,)),
        ],
        compiler_params=pltpu.CompilerParams(vmem_limit_bytes=60_000_000),
    )(*results)
    return down_grad, gate_grad.T, up_grad.T


def solution(mesh):
    torus = Mesh(mesh.devices.reshape(4, 2, 4, 2, 2), AXES)
    fsdp, tensor = ("x", "yl"), ("z", "yh", "c")
    in_specs = (
        P(fsdp),
        P(fsdp, tensor),
        P(fsdp, tensor),
        P(fsdp, tensor),
        P(None, tensor, fsdp),
    )
    out_specs = (P(None, tensor, fsdp), P(fsdp, tensor), P(fsdp, tensor))
    return jax.shard_map(
        shards, mesh=torus, in_specs=in_specs, out_specs=out_specs, check_vma=False
    )
```

```python
import jax
import jax.numpy as jnp
from jax import lax
from jax.experimental import pallas as pl
from jax.experimental.pallas import tpu as pltpu
from jax.sharding import Mesh
from jax.sharding import PartitionSpec as P

AXES = ("x", "yl", "z", "yh", "c")
MESH = pl.DeviceIdType.MESH
F32, BF16 = jnp.float32, jnp.bfloat16
S1, Z1, YH, UP0, UP1, DN0, DN1, FUP, FDN, CC = 0, 4, 8, 12, 16, 20, 24, 28, 32, 36
WW, MM, HR, HL, HFR, HFL = 68, 80, 87, 91, 95, 99
TR, TL, DR1, DL1, DR2, DL2, DW, SEMS = 103, 107, 111, 115, 119, 123, 127, 130


def dot_nt(a, b):
    return lax.dot_general(a, b, (((1,), (1,)), ((), ())), preferred_element_type=F32)


def kernel(
    mod_ref, og_ref, gate_ref, up_ref, w_ref, own_ref, theirs_ref, factor_ref, gg_ref, ug_ref,
    zin_ref, s_ref, wv_ref, ht_ref, part_ref, from_left, from_right, hop_left, hop_right,
    acc_ref, dw_ref, early_ref, out_half, own_v, gate_v, up_v, mod_all, kind_ref,
    send, recv, local,
):
    x, yl, z, yh, c = (lax.axis_index(a) for a in AXES)
    ff, rows = gate_ref.shape
    quarter, cols = rows // 4, og_ref.shape[1]
    half = 2 * cols
    total = rows * 8
    cut = (ff // 2 + 15) // 16 * 16
    top, low = pl.ds(0, cut), pl.ds(cut, ff - cut)
    right, left, across = (x + 1) % 4, (x + 3) % 4, (x + 2) % 4
    up_z, down_z = (z + 1) % 4, (z + 3) % 4
    diagonal = x == z

    barrier = pltpu.get_barrier_semaphore()
    group_steps = [(s // 2, s % 2) for s in range(1, 8)]
    for dx, dy in group_steps:
        pl.semaphore_signal(
            barrier, inc=1, device_id={"x": (x + dx) % 4, "yl": (yl + dy) % 2}, device_id_type=MESH
        )
    for d in range(1, 4):
        pl.semaphore_signal(barrier, inc=1, device_id={"z": (z + d) % 4}, device_id_type=MESH)
    pl.semaphore_signal(barrier, inc=1, device_id={"yh": 1 - yh}, device_id_type=MESH)
    pl.semaphore_signal(barrier, inc=1, device_id={"c": 1 - c}, device_id_type=MESH)

    def rc(src, dst, si, ri, **where):
        return pltpu.make_async_remote_copy(
            src_ref=src, dst_ref=dst, send_sem=send.at[si], recv_sem=recv.at[ri],
            device_id=where, device_id_type=MESH,
        )

    def turn(i):
        return 3 * i + 3 * (i // 2) + 2 * (i // 3)

    def order(k):
        return (z + turn(k)) % 4

    def source(j):
        return (x + turn(j)) % 4

    def tile(i, n):
        return pl.ds(pl.multiple_of(i * n, n), n)

    def each(n, body, start=0):
        def step(i, _):
            body(i)
            return 0

        lax.fori_loop(start, n, step, 0)

    loads = [
        pltpu.make_async_copy(gate_ref, gate_v, local.at[0]),
        pltpu.make_async_copy(up_ref, up_v, local.at[1]),
    ]
    group = x * 2 + yl
    kinds_in = pltpu.make_async_copy(mod_ref, mod_all.at[group], local.at[5])
    kinds_in.start()
    for copy in loads:
        copy.start()

    fourth = (ff // 4 + 15) // 16 * 16
    w_parts = [
        (m, pl.ds(i * fourth, fourth if i < 3 else ff - 3 * fourth))
        for m in range(3) for i in range(4)
    ]

    def w_piece(i, side):
        m, at = w_parts[i]
        return wv_ref.at[m, at, tile(side, half)]

    def w_copy(i):
        m, at = w_parts[i]
        return rc(w_ref.at[m, at, :], w_piece(i, yl), WW + i, WW + i, yl=1 - yl)

    def send_weights(first, last):
        for i in range(first, last):
            w_copy(i).start()

    def w_local(m):
        return pltpu.make_async_copy(w_ref.at[m], wv_ref.at[m, :, tile(yl, half)], local.at[2 + m])

    for m in range(3):
        w_local(m).start()

    def make_hidden(k):
        q = order(k)
        g = gate_v[:, tile(q, quarter)].astype(F32)
        u = up_v[:, tile(q, quarter)].astype(F32)
        ht_ref[q, :, tile(x, quarter)] = (g * jax.nn.sigmoid(g) * u).astype(BF16)

    pl.semaphore_wait(barrier, 12)

    def s_first(q, src):
        return s_ref.at[q, tile(src, quarter), tile(yh * 2 + c, cols)]

    def along_z(d, direct):
        q = (z + d) % 4
        src = og_ref.at[tile(q, quarter), :]
        if direct:
            return rc(src, s_first(q, x), Z1 + d, S1 + x, z=q)
        return rc(src, zin_ref.at[d], Z1 + d, Z1 + d, z=q)

    def home():
        return rc(og_ref.at[tile(z, quarter), :], s_first(z, x), Z1, S1 + x, x=z)

    def along_x(d):
        return rc(zin_ref.at[d], s_first(z, x), S1 + d, S1 + x, x=(z + 4 - d) % 4)

    def passes(d):
        return (z + 4 - d) % 4 != x

    @pl.when(diagonal)
    def _():
        for d in (1, 3, 2):
            along_z(d, True).start()
        pltpu.make_async_copy(
            og_ref.at[tile(z, quarter), :], s_first(z, x), recv.at[S1 + x]
        ).start()

    @pl.when(jnp.logical_not(diagonal))
    def _():
        for d in (1, 3, 2):
            along_z(d, False).start()
        home().start()

    send_weights(0, 4)

    def kinds_copy(i):
        dx, dy = group_steps[i]
        return rc(mod_ref, mod_all.at[group], MM + i, MM + i, x=(x + dx) % 4, yl=(yl + dy) % 2)

    def h_block(q, src):
        return ht_ref.at[q, :, tile(src, quarter)]

    def h_right(k):
        return rc(h_block(order(k), x), h_block(order(k), x), HR + k, HR + k, x=right)

    def h_left(k):
        return rc(h_block(order(k), x), h_block(order(k), x), HL + k, HL + k, x=left)

    def h_on_right(k):
        block = ht_ref.at[order(k), top, tile(left, quarter)]
        return rc(block, block, HFR + k, HFR + k, x=right)

    def h_on_left(k):
        block = ht_ref.at[order(k), low, tile(right, quarter)]
        return rc(block, block, HFL + k, HFL + k, x=left)

    def send_hidden(k):
        h_right(k).start()
        h_left(k).start()

    for copy in loads:
        copy.wait()
    each(1, make_hidden)
    send_hidden(0)
    for i in range(7):
        kinds_copy(i).start()
    for d in (1, 3, 2):
        @pl.when(passes(d))
        def _():
            rc(zin_ref.at[d], zin_ref.at[d], Z1 + d, Z1 + d, z=z).wait_recv()
            along_x(d).start()

    make_hidden(1)

    send_hidden(1)

    def piece(q, e, core, j):
        return s_ref.at[q, tile(source(j), quarter), tile(((yh + e) % 2) * 2 + core, cols)]

    def swap(e, j):
        return rc(piece(z, e, c, j), piece(z, e, c, j), YH + j, YH + j, yh=1 - yh)

    def ring(q, e, j, base, to):
        return rc(piece(q, e, c, j), piece(q, e, c, j), base + j, base + j, z=to)

    def share(k, e, j, core):
        i = CC + 8 * k + 4 * e + j
        return rc(piece(order(k), e, core, j), piece(order(k), e, core, j), i, i, c=1 - c)

    def passed(q, e, j, to_up):
        return ring(q, e, j, FUP + 2 * e, up_z) if to_up else ring(q, e, j, FDN + 2 * e - 2, down_z)

    def pass_on(e, j):
        if j < 2:
            passed(down_z, e, j, True).start()
        else:
            passed(up_z, e, j, False).start()

    def spread_own(j):
        dst = s_first(z, source(j))
        rc(dst, dst, S1, S1 + source(j), x=right).wait_recv()
        swap(0, j).start()
        ring(z, 0, j, UP0, up_z).start()
        ring(z, 0, j, DN0, down_z).start()
        share(0, 0, j, c).start()

    spread_own(0)
    send_weights(4, 4)
    each(4, spread_own, 1)
    send_weights(4, 12)

    def pass_hidden(k):
        q = order(k)
        rc(h_block(q, left), h_block(q, left), HR + k, HR + k, x=right).wait_recv()
        h_on_right(k).start()
        rc(h_block(q, right), h_block(q, right), HL + k, HL + k, x=left).wait_recv()
        h_on_left(k).start()

    each(4, make_hidden, 2)
    pass_hidden(0)
    send_hidden(2)

    def spread_other(j):
        swap(1, j).wait_recv()
        ring(z, 1, j, UP1, up_z).start()
        ring(z, 1, j, DN1, down_z).start()
        share(0, 1, j, c).start()
        ring(down_z, 0, j, UP0, up_z).wait_recv()
        share(1, 0, j, c).start()
        ring(up_z, 0, j, DN0, down_z).wait_recv()
        share(2, 0, j, c).start()
        pass_on(0, j)

    for j in range(4):
        spread_other(j)
    pass_hidden(1)
    send_hidden(3)

    kinds_in.wait()
    for i in range(7):
        dx, dy = group_steps[i]
        src = ((x + 4 - dx) % 4) * 2 + (yl + dy) % 2
        rc(mod_ref, mod_all.at[src], MM, MM + i, x=right).wait_recv()
    for q in range(4):
        pieces = []
        for src in range(4):
            one = mod_all[src * 2 + yl]
            pieces += [one[2 * q : 2 * q + 1, :], one[2 * q + 1 : 2 * q + 2, :]]
        kind_ref[q] = jnp.concatenate(pieces, axis=1)
    everyone = mod_all[...].reshape(rows // 128 * 8, 128)
    factors = []
    for m in range(3):
        hits = (everyone == m).astype(F32)
        count = jnp.sum(jnp.sum(hits, axis=0, keepdims=True), axis=1, keepdims=True)
        factors.append(total / (3.0 * count))
        factor_ref[m : m + 1, :] = jnp.broadcast_to(factors[m], (1, 128))

    def block_in(k):
        def one(i):
            share(k, i // 4, i % 4, 1 - c).wait_recv()

        each(8, one)

    def hidden_in(k):
        q = order(k)
        a = ht_ref.at[q, top, tile(across, quarter)]
        rc(a, a, HFR + k, HFR + k, x=right).wait_recv()
        b = ht_ref.at[q, low, tile(across, quarter)]
        rc(b, b, HFL + k, HFL + k, x=left).wait_recv()

    def marked(q, m):
        return ht_ref[q] * (kind_ref[q] == m).astype(F32).astype(BF16)

    def add_quarter(k, opening=False):
        q = order(k)
        block_in(k)
        hidden_in(k)

        def one(m):
            rows_marked = marked(q, m)
            for ref, side in ((acc_ref, 1 - yl), (dw_ref, yl)):
                part = jnp.dot(
                    rows_marked, s_ref[q, :, tile(side, half)], preferred_element_type=F32
                )
                ref[m] = part if opening else ref[m] + part

        each(3, one)

    def spread_near(j):
        ring(up_z, 1, j, DN1, down_z).wait_recv()
        share(2, 1, j, c).start()
        ring(down_z, 1, j, UP1, up_z).wait_recv()
        share(1, 1, j, c).start()
        pass_on(1, j)

    far = (z + 2) % 4

    def spread_far(j):
        for e in range(2):
            passed(far, e, j, j < 2).wait_recv()
            share(3, e, j, c).start()

    def two_blocks(p):
        return (x + 2 + p) % 4, (x + 1 + 3 * p) % 4

    def d_hidden_part(q, p, at):
        one, two = two_blocks(p)
        block = jnp.concatenate(
            [s_ref[q, tile(one, quarter), at], s_ref[q, tile(two, quarter), at]], axis=0
        )
        kind = jnp.concatenate(
            [kind_ref[q, :, tile(one, quarter)], kind_ref[q, :, tile(two, quarter)]], axis=1
        )
        got = dot_nt(wv_ref[0, :, at], block)
        for m in range(1, 3):
            got = jnp.where(kind == m, dot_nt(wv_ref[m, :, at], block), got)
        return got

    def early(p):
        early_ref[p] = d_hidden_part(z, p, tile(yl, half))

    add_quarter(0, True)
    for j in range(4):
        spread_near(j)
    for m in range(3):
        w_local(m).wait()
    each(2, early)
    pass_hidden(2)
    add_quarter(1)
    for j in range(4):
        spread_far(j)
    pass_hidden(3)
    add_quarter(2)
    for i in range(12):
        theirs = w_piece(i, 1 - yl)
        rc(theirs, theirs, WW + i, WW + i, yl=1 - yl).wait_recv()

    def hop(k, to_right):
        q = order(k)
        if to_right:
            return rc(part_ref.at[across, q, top, :], hop_left.at[k], TR + k, TR + k, x=right)
        return rc(part_ref.at[across, q, low, :], hop_right.at[k], TL + k, TL + k, x=left)

    def give(k, to_right, rows_at, base):
        q = order(k)
        if to_right:
            return rc(part_ref.at[right, q, rows_at, :], from_left.at[k, rows_at, :],
                      base + k, base + k, x=right)
        return rc(part_ref.at[left, q, rows_at, :], from_right.at[k, rows_at, :],
                  base + k, base + k, x=left)

    def gives(k, i):
        return give(k, i % 2 == 0, (low, top, top, low)[i], (DR1, DL1, DR2, DL2)[i])

    def relay(k):
        q = order(k)
        hop(k, True).wait_recv()
        part_ref[right, q, top, :] = (
            part_ref[right, q, top, :].astype(F32) + hop_left[k].astype(F32)
        ).astype(BF16)
        gives(k, 2).start()
        hop(k, False).wait_recv()
        part_ref[left, q, low, :] = (
            part_ref[left, q, low, :].astype(F32) + hop_right[k].astype(F32)
        ).astype(BF16)
        gives(k, 3).start()

    def keep(q, p, got):
        got = got.astype(BF16)
        one, two = two_blocks(p)
        part_ref[one, q] = got[:, :quarter]
        part_ref[two, q] = got[:, quarter:]

    def send_first(k):
        hop(k, True).start()
        hop(k, False).start()
        gives(k, 0).start()

    def first_pair(p):
        keep(z, p, early_ref[p] + d_hidden_part(z, p, tile(1 - yl, half)))

        @pl.when(p == 0)
        def _():
            send_first(0)

    def d_hidden(k):
        q = order(k)

        def pair(p):
            keep(q, p, d_hidden_part(q, p, slice(None)))

            @pl.when(p == 0)
            def _():
                send_first(k)
                relay(k - 1)

        each(2, pair)
        gives(k, 1).start()

    def dw_copy(m):
        return rc(out_half.at[m], theirs_ref.at[m], DW + m, DW + m, yl=1 - yl)

    def last_sum(ref, m, side):
        q = order(3)
        return ref[m] + jnp.dot(
            marked(q, m), s_ref[q, :, tile(side, half)], preferred_element_type=F32
        )

    def own_out(m):
        return pltpu.make_async_copy(own_v.at[m], own_ref.at[m], local.at[6 + m])

    def grads_out(k):
        at = tile(order(k), quarter)
        return (
            pltpu.make_async_copy(up_v.at[:, at], ug_ref.at[:, at], local.at[9 + k]),
            pltpu.make_async_copy(gate_v.at[:, at], gg_ref.at[:, at], local.at[13 + k]),
        )

    def other_half(m):
        out_half[m] = last_sum(acc_ref, m, 1 - yl).astype(BF16)
        dw_copy(m).start()

    def own_half(m):
        own_v[m] = last_sum(dw_ref, m, yl).astype(BF16)
        own_out(m).start()

    block_in(3)
    hidden_in(3)
    other_half(0)
    each(2, first_pair)
    gives(0, 1).start()

    def steady(k):
        @pl.when(k < 3)
        def _():
            other_half(k)

        d_hidden(k)

    each(4, steady, 1)
    each(1, own_half)
    relay(3)
    each(3, own_half, 1)

    def finish(k):
        q = order(k)
        for i in range(4):
            gives(k, i).wait_recv()
        kind = kind_ref[q, :, tile(x, quarter)]
        scale = jnp.where(kind == 0, factors[0], jnp.where(kind == 1, factors[1], factors[2]))
        t = scale * (
            part_ref[x, q].astype(F32) + from_left[k].astype(F32) + from_right[k].astype(F32)
        )
        g = gate_v[:, tile(q, quarter)].astype(F32)
        u = up_v[:, tile(q, quarter)].astype(F32)
        s = jax.nn.sigmoid(g)
        up_v[:, tile(q, quarter)] = (t * (g * s)).astype(BF16)
        gate_v[:, tile(q, quarter)] = (t * u * (s * (1.0 + g * (1.0 - s)))).astype(BF16)
        for copy in grads_out(k):
            copy.start()

    each(4, finish)
    for m in range(3):
        own_out(m).wait()
        dw_copy(m).wait_recv()

    @pl.when(diagonal)
    def _():
        for d in range(1, 4):
            along_z(d, True).wait_send()

    @pl.when(jnp.logical_not(diagonal))
    def _():
        for d in range(1, 4):
            along_z(d, False).wait_send()
        home().wait_send()

    for d in range(1, 4):
        @pl.when(passes(d))
        def _():
            along_x(d).wait_send()

    for i in range(7):
        kinds_copy(i).wait_send()

    def drain(k):
        for copy in grads_out(k):
            copy.wait()
        swap(0, k).wait_send()
        for q, e, base, to in (
            (z, 0, UP0, up_z), (z, 1, UP1, up_z), (z, 0, DN0, down_z),
            (z, 1, DN1, down_z),
        ):
            ring(q, e, k, base, to).wait_send()
        for copy in (h_right(k), h_left(k), h_on_right(k), h_on_left(k)):
            copy.wait_send()
        for i in range(8):
            share(k, i // 4, i % 4, c).wait_send()
        for copy in (hop(k, True), hop(k, False)):
            copy.wait_send()
        for i in range(4):
            gives(k, i).wait_send()

    for e in range(2):
        for j in range(4):
            passed((down_z, up_z)[j // 2], e, j, j < 2).wait_send()
    each(4, drain)
    for i in range(12):
        w_copy(i).wait_send()
    for m in range(3):
        dw_copy(m).wait_send()


def store(
    own_ref, theirs_ref, factor_ref, gg_ref, ug_ref, dw_out, gg_out, ug_out,
    own_v, theirs_v, dw_v, gg_v, ug_v, come, go,
):
    ff = gg_ref.shape[0]
    cut = (ff // 2 + 15) // 16 * 16
    parts = [(m, at) for m in range(3) for at in (pl.ds(0, cut), pl.ds(cut, ff - cut))]
    copy = pltpu.make_async_copy
    grads_in = [copy(gg_ref, gg_v, come.at[0]), copy(ug_ref, ug_v, come.at[1])]
    grads_go = [copy(gg_v, gg_out, go.at[0]), copy(ug_v, ug_out, go.at[1])]
    sums_in = [
        (
            copy(own_ref.at[m, at, :], own_v.at[m, at, :], come.at[2 + 2 * i]),
            copy(theirs_ref.at[m, at, :], theirs_v.at[m, at, :], come.at[3 + 2 * i]),
        )
        for i, (m, at) in enumerate(parts)
    ]
    sums_go = [
        copy(dw_v.at[m, at, :], dw_out.at[m, at, :], go.at[2 + i]) for i, (m, at) in enumerate(parts)
    ]
    for one in grads_in:
        one.start()
    for pair in sums_in:
        for one in pair:
            one.start()
    for i in range(2):
        grads_in[i].wait()
        grads_go[i].start()
    for i, (m, at) in enumerate(parts):
        for one in sums_in[i]:
            one.wait()
        dw_v[m, at, :] = (own_v[m, at, :].astype(F32) + theirs_v[m, at, :].astype(F32)) * (
            factor_ref[m : m + 1, :1]
        )
        sums_go[i].start()
    for one in grads_go + sums_go:
        one.wait()


def shards(modality, out_grad, gate_pre, up_pre, down_weight):
    rows, cols = out_grad.shape
    kinds, ff, half = down_weight.shape
    quarter = rows // 4
    cut = (ff // 2 + 15) // 16 * 16
    hbm = pl.BlockSpec(memory_space=pltpu.HBM)
    vmem = pl.BlockSpec(memory_space=pltpu.VMEM)
    grad_shapes = (jax.ShapeDtypeStruct((ff, rows), BF16),) * 2
    shapes = (
        jax.ShapeDtypeStruct((kinds, ff, half), BF16),
        jax.ShapeDtypeStruct((kinds, ff, half), BF16),
        jax.ShapeDtypeStruct((kinds, 128), F32),
        *grad_shapes,
    )
    results = pl.pallas_call(
        kernel,
        out_shape=shapes,
        in_specs=[hbm] * 5,
        out_specs=(hbm, hbm, vmem, hbm, hbm),
        scratch_shapes=[
            pltpu.VMEM((4, quarter, cols), BF16),
            pltpu.VMEM((4, rows, 4 * cols), BF16),
            pltpu.VMEM((kinds, ff, 2 * half), BF16),
            pltpu.VMEM((4, ff, rows), BF16),
            pltpu.VMEM((4, 4, ff, quarter), BF16),
            pltpu.VMEM((4, ff, quarter), BF16),
            pltpu.VMEM((4, ff, quarter), BF16),
            pltpu.VMEM((4, cut, quarter), BF16),
            pltpu.VMEM((4, ff - cut, quarter), BF16),
            pltpu.VMEM((kinds, ff, half), F32),
            pltpu.VMEM((kinds, ff, half), F32),
            pltpu.VMEM((2, ff, half), F32),
            pltpu.VMEM((kinds, ff, half), BF16),
            pltpu.VMEM((kinds, ff, half), BF16),
            pltpu.VMEM((ff, rows), BF16),
            pltpu.VMEM((ff, rows), BF16),
            pltpu.VMEM((8, rows // 128, 128), jnp.int32),
            pltpu.VMEM((4, 1, rows), jnp.int32),
            pltpu.SemaphoreType.DMA((SEMS,)),
            pltpu.SemaphoreType.DMA((SEMS,)),
            pltpu.SemaphoreType.DMA((17,)),
        ],
        compiler_params=pltpu.CompilerParams(
            collective_id=0, has_side_effects=True, vmem_limit_bytes=60_000_000
        ),
    )(modality.reshape(rows // 128, 128), out_grad, gate_pre.T, up_pre.T, down_weight)
    down_grad, gate_grad, up_grad = pl.pallas_call(
        store,
        out_shape=(jax.ShapeDtypeStruct((kinds, ff, half), F32), *grad_shapes),
        in_specs=[hbm, hbm, vmem, hbm, hbm],
        out_specs=(hbm, hbm, hbm),
        scratch_shapes=[
            pltpu.VMEM((kinds, ff, half), BF16),
            pltpu.VMEM((kinds, ff, half), BF16),
            pltpu.VMEM((kinds, ff, half), F32),
            pltpu.VMEM((ff, rows), BF16),
            pltpu.VMEM((ff, rows), BF16),
            pltpu.SemaphoreType.DMA((14,)),
            pltpu.SemaphoreType.DMA((8,)),
        ],
        compiler_params=pltpu.CompilerParams(vmem_limit_bytes=60_000_000),
    )(*results)
    return down_grad, gate_grad.T, up_grad.T


def solution(mesh):
    torus = Mesh(mesh.devices.reshape(4, 2, 4, 2, 2), AXES)
    fsdp, tensor = ("x", "yl"), ("z", "yh", "c")
    in_specs = (
        P(fsdp),
        P(fsdp, tensor),
        P(fsdp, tensor),
        P(fsdp, tensor),
        P(None, tensor, fsdp),
    )
    out_specs = (P(None, tensor, fsdp), P(fsdp, tensor), P(fsdp, tensor))
    return jax.shard_map(
        shards, mesh=torus, in_specs=in_specs, out_specs=out_specs, check_vma=False
    )
```
